32 devices in a mesh: groups: 2 (over x), gx: 16 (over z, y, core).
Axes of the slice: x: 2, y: 2, z: 4, core: 2. Of those that a mesh axis runs over, the one named last changes fastest.
Arguments:
- tokens: bfloat16 [512, 8192], P('groups', 'gx'), parts along dimension 0, may hold values from -6 to 6
- gate_weight: bfloat16 [8192, 14336], P(None, 'gx'), may hold values from -0.09375 to 0.09375
- up_weight: bfloat16 [8192, 14336], P(None, 'gx'), may hold values from -0.09375 to 0.09375
- down_weight: bfloat16 [14336, 8192], P('gx'), may hold values from -0.0625 to 0.0625
Outputs:
- mixed: bfloat16 [512, 8192], P('groups', 'gx'), parts along dimension 0
The draws below stay inside these ranges and needn't reach their ends.
There are 2 independent parts, one for each index of `groups`. The reference program is written for one: setup_inputs(seed, part) draws one part's arguments, and reference() takes and returns one part's arrays. A program takes and returns all parts, laid end to end along the dimension named above; an argument that names none is the same for every part. Nothing has to cross between parts.
All inputs are finite; a program needn't handle non-finite values.
Results may differ from the reference program's by a relative error of at most 0.0049.
Values may be sent and summed in bfloat16 or wider, within the bound.
A program may use at most 128 MiB of HBM per device.

```python
import jax
import jax.numpy as jnp

D = 8192
FF = 14336
TOK = 256


def with_spikes(drawn, rng, source, target, parts, factor):
    def block_of(dim):
        return (jnp.arange(drawn.shape[dim]) // (drawn.shape[dim] // parts)).reshape((-1,) + (1,) * (drawn.ndim - 1 - dim))

    one_side = jax.random.permutation(rng, parts)[block_of(target)]
    other_side = (block_of(target) + parts // 2) % parts
    return jnp.where((block_of(source) == one_side) | (block_of(source) == other_side), factor * drawn, drawn)


def block_levels(own_key, extent, shards, least, high):
    def one(dim, shards_of):
        draws = jax.random.uniform(jax.random.fold_in(jax.random.fold_in(own_key, 6), dim), (shards_of,), jnp.float32, least / len(shards), high / len(shards))
        return jnp.repeat(jnp.exp(draws), extent[dim] // shards_of).reshape((-1,) + (1,) * (len(extent) - dim - 1))

    gain = one(*shards[0])
    for cut in shards[1:]:
        gain = gain * one(*cut)
    return gain


def scatter_about(stream_key, shape, deviation, limit, split=(), dtype=jnp.bfloat16):
    drawn = deviation * jax.random.normal(stream_key, shape, jnp.float32)
    if split:
        drawn = drawn * block_levels(stream_key, shape, split, -0.22, 0.18)
    return jnp.clip(drawn, -limit, limit).astype(dtype)


def heavy_noise(own_key, dims, scale, bound, split, heavy, held_as=jnp.bfloat16):
    values = scale * jax.random.normal(own_key, dims, jnp.float32)
    if split:
        values = values * block_levels(own_key, dims, split, -0.22, 0.18)
    return jnp.clip(with_spikes(values, jax.random.fold_in(own_key, 3), *heavy), -bound, bound).astype(held_as)


def setup_inputs(seed: int = 0, part: int = 0) -> dict:
    splits = jax.random.split(jax.random.key(seed), 5)
    own_keys = jax.random.split(jax.random.fold_in(splits[4], part), 5)
    return {
        "tokens": scatter_about(own_keys[0], (TOK, D), 1.0, 6.0, ((1, 16),)),
        "gate_weight": heavy_noise(splits[1], (D, FF), D ** -0.5, 0.09375, ((1, 16),), (0, 1, 16, 2.0)),
        "up_weight": heavy_noise(splits[2], (D, FF), D ** -0.5, 0.09375, ((1, 16),), (0, 1, 16, 2.0)),
        "down_weight": heavy_noise(splits[3], (FF, D), FF ** -0.5, 0.0625, ((0, 16),), (0, 1, 16, 2.0)),
    }


def reference(tokens, gate_weight, up_weight, down_weight):
    gate = jnp.dot(tokens, gate_weight, preferred_element_type=jnp.float32)
    up = jnp.dot(tokens, up_weight, preferred_element_type=jnp.float32)
    hidden = (jax.nn.silu(gate) * up).astype(jnp.bfloat16)
    return jnp.dot(hidden, down_weight, preferred_element_type=jnp.float32).astype(jnp.bfloat16)
```

```python
import functools

import jax
import jax.numpy as jnp
from jax import lax
from jax.experimental import pallas as pl
from jax.experimental.pallas import tpu as pltpu
from jax.sharding import PartitionSpec as P

MESH = pl.DeviceIdType.MESH
VMEM_LIMIT = 67043328


def kernel(
    n, width, tok_hbm, gate_hbm, up_hbm, down_hbm, out_ref,
    tok, wg, wu, wd, acc_g, acc_u, hid, own, sout, sin, rin, rout,
    tok_sem, w_sem, d_sem, ag_send, ag_recv, sib_send, sib_recv,
    pair_send, pair_recv, rs_send, rs_recv,
):
    half = n // 2
    token_rows, block = tok_hbm.shape
    hrows = token_rows // 2
    long = n // width
    me = lax.axis_index("gx")
    core = lax.rem(me, 2)
    chip = me // 2
    z = chip // width
    y = chip - z * width
    r = z + y * (n - 1 - 2 * z)

    def device_at(pos, c):
        pos = lax.rem(pos + n, n)
        yy = pos // long
        zz = pos + yy * (n - 1 - 2 * pos)
        return (zz * width + yy) * 2 + c

    sib = me + 1 - 2 * core
    target = (device_at(r + 1, core), device_at(r - 1, core))

    def rows(h):
        return pl.ds(h * hrows, hrows)

    def slot(k, d, cr):
        if k == 0:
            return cr
        if k < half:
            return 2 + (k - 1) * 4 + d * 2 + cr
        return 2 + (half - 1) * 4 + cr

    def step_slots(k):
        dirs = (0, 1) if 0 < k < half else (0,)
        return [(d, cr, slot(k, d, cr)) for d in dirs for cr in (0, 1)]

    sends = []

    def remote(src, dst, s_sem, r_sem, dev):
        return pltpu.make_async_remote_copy(
            src_ref=src, dst_ref=dst, send_sem=s_sem, recv_sem=r_sem,
            device_id={"gx": dev}, device_id_type=MESH,
        )

    def send(*args):
        copy = remote(*args)
        copy.start()
        sends.append(copy)

    def weight_copies(s, dev):
        part = pl.ds(pl.multiple_of(dev * block, block), block)
        return (
            pltpu.make_async_copy(gate_hbm.at[part], wg.at[s], w_sem.at[0, s]),
            pltpu.make_async_copy(up_hbm.at[part], wu.at[s], w_sem.at[1, s]),
        )

    def start_weights(k):
        for d, cr, s in step_slots(k):
            pos = r - k if d == 0 else r + k
            c = core if cr == 0 else 1 - core
            for copy in weight_copies(s, device_at(pos, c)):
                copy.start()

    def down_copy(q, cr):
        c = core if cr == 0 else 1 - core
        dev = device_at(r + q, c)
        part = pl.ds(pl.multiple_of(dev * block, block), block)
        s = 2 * q + cr
        return pltpu.make_async_copy(down_hbm.at[:, part], wd.at[s], d_sem.at[s])

    def add_block(s):
        for copy in weight_copies(s, 0):
            copy.wait()
        x = tok[s]
        acc_g[...] += jnp.dot(x, wg[s], preferred_element_type=jnp.float32)
        acc_u[...] += jnp.dot(x, wu[s], preferred_element_type=jnp.float32)

    def add_step(k, cr):
        slots = [s for _, c, s in step_slots(k) if c == cr]
        if len(slots) == 1:
            add_block(slots[0])
        else:
            @pl.loop(0, 2)
            def _(i):
                add_block(slots[0] + 2 * i)

    first = pltpu.make_async_copy(tok_hbm, tok.at[0], tok_sem)
    first.start()
    barrier = pltpu.get_barrier_semaphore()
    for dev in (*target, sib):
        pl.semaphore_signal(barrier, inc=1, device_id={"gx": dev}, device_id_type=MESH)
    start_weights(0)
    start_weights(1)
    acc_g[...] = jnp.zeros_like(acc_g)
    acc_u[...] = jnp.zeros_like(acc_u)
    first.wait()
    pl.semaphore_wait(barrier, 3)

    def ring_copy(k, d, h):
        src = tok.at[slot(k - 1, d, 0), rows(h)]
        dst = tok.at[slot(k, d, 0), rows(h)]
        return src, dst, ag_send.at[d, k, h], ag_recv.at[d, k, h], target[d]

    def pair_copy(k, d, h):
        src = tok.at[slot(k, d, 0), rows(h)]
        dst = tok.at[slot(k, d, 1), rows(h)]
        return src, dst, sib_send.at[d, k, h], sib_recv.at[d, k, h], sib

    for part in (0, 1):
        for d in (0, 1):
            send(*ring_copy(1, d, d if part == 0 else 1 - d))
    for h in (0, 1):
        send(*pair_copy(0, 0, h))
    for k in range(1, half + 1):
        if k < half:
            start_weights(k + 1)
        qs = [q for q in range(n) if q % half == k - 1]
        for q in qs:
            for cr in (0, 1):
                down_copy(q, cr).start()
        for part in (0, 1):
            for d in (0, 1):
                h = d if part == 0 else 1 - d
                if k == half and part == 1:
                    continue
                remote(*ring_copy(k, d, h)).wait_recv()
                if k + 1 < half or (k + 1 == half and part == 0):
                    send(*ring_copy(k + 1, d, h))
                send(*pair_copy(k, d, h))
            if part == 1:
                for d in (0, 1) if k > 1 else (0,):
                    for h in (0, 1):
                        remote(*pair_copy(k - 1, d, h)).wait_recv()
            add_step(k - 1, part)
    add_step(half, 0)
    for d in (0, 1):
        remote(*pair_copy(half, d, d)).wait_recv()
    add_step(half, 1)

    gate = acc_g[...]
    hid[...] = (gate / (1.0 + jnp.exp(-gate)) * acc_u[...]).astype(hid.dtype)

    def partial(q, cr):
        down_copy(q, cr).wait()
        return jnp.dot(hid[...], wd[2 * q + cr], preferred_element_type=jnp.float32)

    def sib_copy(q):
        return sout.at[q], sin.at[q], pair_send.at[q], pair_recv.at[q], sib

    def for_sib(q):
        sout[q] = partial(q, 1).astype(sout.dtype)
        send(*sib_copy(q))

    def for_own(q):
        own[q] = partial(q, 0)

    seen = set()

    def pair_sum(q, h):
        if q not in seen:
            seen.add(q)
            remote(*sib_copy(q)).wait_recv()
        return own[q, rows(h)] + sin[q, rows(h)].astype(jnp.float32)

    def sum_copy(o, d, h):
        return (rout.at[d, o - 1, h], rin.at[d, o - 1, h],
                rs_send.at[d, o - 1, h], rs_recv.at[d, o - 1, h], target[d])

    def arrived(o, d, h):
        remote(*sum_copy(o + 1, d, h)).wait_recv()
        return rin[d, o, h].astype(jnp.float32)

    def dest(o, d):
        return o % n if d == 0 else (n - o) % n

    def group(o):
        return sorted({dest(o, 0), dest(o, 1)})

    for o in (half, half - 1):
        for q in group(o):
            for_sib(q)
    for_own(half)
    for d in (0, 1):
        rout[d, half - 1, d] = pair_sum(half, d).astype(rout.dtype)
        send(*sum_copy(half, d, d))
    for q in group(half - 1):
        for_own(q)
    for o in range(half - 1, 0, -1):
        for part in (0, 1):
            for d in (0, 1):
                h = 1 - d if part == 0 else d
                total = pair_sum(dest(o, d), h)
                if part == 1 or o < half - 1:
                    total = total + arrived(o, d, h)
                rout[d, o - 1, h] = total.astype(rout.dtype)
                send(*sum_copy(o, d, h))
            if part == 0:
                for q in group(o - 1):
                    for_sib(q)
                for q in group(o - 1):
                    for_own(q)
    for d in (0, 1):
        own[0, rows(1 - d)] = pair_sum(0, 1 - d) + arrived(0, d, 1 - d)
    for d in (0, 1):
        out_ref[rows(d)] = (own[0, rows(d)] + arrived(0, d, d)).astype(out_ref.dtype)
    for copy in sends:
        copy.wait_send()


def on_device(n, width, tokens, gate_weight, up_weight, down_weight):
    token_rows, block = tokens.shape
    hidden = gate_weight.shape[1]
    half = n // 2
    slots = 2 * n
    hrows = token_rows // 2
    bf16, f32 = jnp.bfloat16, jnp.float32
    dma = pltpu.SemaphoreType.DMA
    ring = (2, half + 1, 2)
    return pl.pallas_call(
        functools.partial(kernel, n, width),
        out_shape=jax.ShapeDtypeStruct((token_rows, block), bf16),
        in_specs=[pl.BlockSpec(memory_space=pl.ANY)] * 4,
        out_specs=pl.BlockSpec(memory_space=pltpu.VMEM),
        scratch_shapes=[
            pltpu.VMEM((slots, token_rows, block), bf16),
            pltpu.VMEM((slots, block, hidden), bf16),
            pltpu.VMEM((slots, block, hidden), bf16),
            pltpu.VMEM((slots, hidden, block), bf16),
            pltpu.VMEM((token_rows, hidden), f32),
            pltpu.VMEM((token_rows, hidden), f32),
            pltpu.VMEM((token_rows, hidden), bf16),
            pltpu.VMEM((n, token_rows, block), f32),
            pltpu.VMEM((n, token_rows, block), bf16),
            pltpu.VMEM((n, token_rows, block), bf16),
            pltpu.VMEM((2, half, 2, hrows, block), bf16),
            pltpu.VMEM((2, half, 2, hrows, block), bf16),
            dma(()), dma((2, slots)), dma((slots,)),
            dma(ring), dma(ring), dma(ring), dma(ring),
            dma((n,)), dma((n,)), dma((2, half, 2)), dma((2, half, 2)),
        ],
        compiler_params=pltpu.CompilerParams(
            collective_id=0, has_side_effects=True, vmem_limit_bytes=VMEM_LIMIT
        ),
    )(tokens, gate_weight, up_weight, down_weight)


def solution(mesh):
    n = mesh.shape["gx"] // 2
    spots = {tuple(getattr(dev, "coords", (0, 0, 0)))[:2] for dev in mesh.devices[0]}
    width = len(spots) if len(spots) in (1, 2) else 1
    return jax.shard_map(
        functools.partial(on_device, n, width),
        mesh=mesh,
        in_specs=(P("groups", "gx"), P(None, "gx"), P(None, "gx"), P("gx", None)),
        out_specs=P("groups", "gx"),
        check_vma=False,
    )
```

```python
import functools

import jax
import jax.numpy as jnp
from jax import lax
from jax.experimental import pallas as pl
from jax.experimental.pallas import tpu as pltpu
from jax.sharding import PartitionSpec as P

MESH = pl.DeviceIdType.MESH
VMEM_LIMIT = 67043328


def kernel(
    n, width, tok_hbm, gate_hbm, up_hbm, down_hbm, out_ref,
    tok, wg, wu, wd, acc_g, acc_u, hid, own, sout, sin, rin, rout,
    tok_sem, w_sem, d_sem, ag_send, ag_recv, sib_send, sib_recv,
    pair_send, pair_recv, rs_send, rs_recv,
):
    half = n // 2
    token_rows, block = tok_hbm.shape
    prow = token_rows // 4
    long = n // width
    me = lax.axis_index("gx")
    core = lax.rem(me, 2)
    chip = me // 2
    z = chip // width
    y = chip - z * width
    r = z + y * (n - 1 - 2 * z)

    def device_at(pos, c):
        pos = lax.rem(pos + n, n)
        yy = pos // long
        zz = pos + yy * (n - 1 - 2 * pos)
        return (zz * width + yy) * 2 + c

    sib = me + 1 - 2 * core
    target = (device_at(r + 1, core), device_at(r - 1, core))

    def rows(p):
        return pl.ds(p * prow, prow)

    def span(ph):
        return pl.ds(0, 4 * prow) if ph is None else pl.ds(2 * ph * prow, 2 * prow)

    def piece(ph, part, d):
        return 2 * ph + (d if part == 0 else 1 - d)

    def slot(k, d, cr):
        if k == 0:
            return cr
        if k < half:
            return 2 + (k - 1) * 4 + d * 2 + cr
        return 2 + (half - 1) * 4 + cr

    def step_slots(k):
        dirs = (0, 1) if 0 < k < half else (0,)
        return [(d, cr, slot(k, d, cr)) for d in dirs for cr in (0, 1)]

    sends = []

    def remote(src, dst, s_sem, r_sem, dev):
        return pltpu.make_async_remote_copy(
            src_ref=src, dst_ref=dst, send_sem=s_sem, recv_sem=r_sem,
            device_id={"gx": dev}, device_id_type=MESH,
        )

    def send(*args):
        copy = remote(*args)
        copy.start()
        sends.append(copy)

    def weight_copies(s, dev):
        part = pl.ds(pl.multiple_of(dev * block, block), block)
        return (
            pltpu.make_async_copy(gate_hbm.at[part], wg.at[s], w_sem.at[0, s]),
            pltpu.make_async_copy(up_hbm.at[part], wu.at[s], w_sem.at[1, s]),
        )

    def start_weights(k):
        for d, cr, s in step_slots(k):
            pos = r - k if d == 0 else r + k
            c = core if cr == 0 else 1 - core
            for copy in weight_copies(s, device_at(pos, c)):
                copy.start()

    def down_copy(q, cr):
        c = core if cr == 0 else 1 - core
        dev = device_at(r + q, c)
        part = pl.ds(pl.multiple_of(dev * block, block), block)
        s = 2 * q + cr
        return pltpu.make_async_copy(down_hbm.at[:, part], wd.at[s], d_sem.at[s])

    def add_block(s, ph, fresh):
        if fresh:
            for copy in weight_copies(s, 0):
                copy.wait()
        at = span(ph)
        x = tok[s, at]
        acc_g[at] += jnp.dot(x, wg[s], preferred_element_type=jnp.float32)
        acc_u[at] += jnp.dot(x, wu[s], preferred_element_type=jnp.float32)

    first = pltpu.make_async_copy(tok_hbm, tok.at[0], tok_sem)
    first.start()
    barrier = pltpu.get_barrier_semaphore()
    for dev in (*target, sib):
        pl.semaphore_signal(barrier, inc=1, device_id={"gx": dev}, device_id_type=MESH)
    start_weights(0)
    start_weights(1)
    first.wait()
    pl.semaphore_wait(barrier, 3)

    def ring_copy(k, d, h):
        src = tok.at[slot(k - 1, d, 0), rows(h)]
        dst = tok.at[slot(k, d, 0), rows(h)]
        return src, dst, ag_send.at[d, k, h], ag_recv.at[d, k, h], target[d]

    def pair_copy(k, d, h):
        src = tok.at[slot(k, d, 0), rows(h)]
        dst = tok.at[slot(k, d, 1), rows(h)]
        return src, dst, sib_send.at[d, k, h], sib_recv.at[d, k, h], sib

    def move(ph, part, k):
        for d in (0, 1):
            p = piece(ph, part, d)
            if k > 1:
                remote(*ring_copy(k - 1, d, p)).wait_recv()
            if k < half or (k == half and part == 0):
                send(*ring_copy(k, d, p))
            if k > 1:
                send(*pair_copy(k - 1, d, p))

    came = set()

    def add_step(k, cr, ph):
        if cr == 1:
            phases = (0, 1) if ph is None else (ph,)
            for d, c, s in step_slots(k):
                for p in [2 * a + b for a in phases for b in (0, 1)]:
                    if c == 1:
                        way = p % 2 if k == half else d
                        remote(*pair_copy(k, way, p)).wait_recv()
        slots = [s for _, c, s in step_slots(k) if c == cr]
        fresh = (k, cr) not in came
        came.add((k, cr))
        if len(slots) == 1:
            add_block(slots[0], ph, fresh)
        else:
            @pl.loop(0, 2)
            def _(i):
                add_block(slots[0] + 2 * i, ph, fresh)

    def activate(ph):
        at = span(ph)
        gate = acc_g[at]
        hid[at] = (gate / (1.0 + jnp.exp(-gate)) * acc_u[at]).astype(hid.dtype)

    loaded = set()

    def partial(q, cr, ph):
        if (q, cr) not in loaded:
            loaded.add((q, cr))
            down_copy(q, cr).wait()
        return jnp.dot(hid[span(ph)], wd[2 * q + cr], preferred_element_type=jnp.float32)

    def sib_copy(q, ph):
        at = span(ph)
        return sout.at[q, at], sin.at[q, at], pair_send.at[q, ph], pair_recv.at[q, ph], sib

    def for_sib(q, ph):
        sout[q, span(ph)] = partial(q, 1, ph).astype(sout.dtype)
        send(*sib_copy(q, ph))

    def for_own(q, ph):
        own[q, span(ph)] = partial(q, 0, ph)

    seen = set()

    def pair_sum(q, p):
        if (q, p // 2) not in seen:
            seen.add((q, p // 2))
            remote(*sib_copy(q, p // 2)).wait_recv()
        return own[q, rows(p)] + sin[q, rows(p)].astype(jnp.float32)

    def sum_copy(o, d, p):
        return (rout.at[d, o - 1, p], rin.at[d, o - 1, p],
                rs_send.at[d, o - 1, p], rs_recv.at[d, o - 1, p], target[d])

    def arrived(o, d, p):
        remote(*sum_copy(o + 1, d, p)).wait_recv()
        return rin[d, o, p].astype(jnp.float32)

    def dest(o, d):
        return o % n if d == 0 else (n - o) % n

    def group(o):
        return sorted({dest(o, 0), dest(o, 1)})

    def project(o, ph):
        for q in group(o):
            for_sib(q, ph)
        for q in group(o):
            for_own(q, ph)

    def pass_sum(ph, part, o):
        for d in (0, 1):
            p = piece(ph, part, d)
            total = pair_sum(dest(o, d), p)
            if o < half - 1 or (o == half - 1 and part == 0):
                total = total + arrived(o, d, p)
            rout[d, o - 1, p] = total.astype(rout.dtype)
            send(*sum_copy(o, d, p))

    def finish(ph):
        for d in (0, 1):
            p = piece(ph, 1, d)
            own[0, rows(p)] = pair_sum(0, p) + arrived(0, d, p)
        for d in (0, 1):
            p = piece(ph, 0, d)
            out_ref[rows(p)] = (own[0, rows(p)] + arrived(0, d, p)).astype(out_ref.dtype)

    def start_down(os):
        for q in [q for o in os for q in group(o)]:
            for cr in (0, 1):
                down_copy(q, cr).start()

    spare = [(part, k) for k in range(1, half) for part in (0, 1)] + [(0, half)]
    for k in range(1, half):
        move(0, 0, k)
        move(0, 1, k)
        if k == 1:
            for p in range(4):
                send(*pair_copy(0, 0, p))
        move(1, *spare[k - 1])
        start_weights(k + 1)
        if k == 1:
            acc_g[...] = jnp.zeros_like(acc_g)
            acc_u[...] = jnp.zeros_like(acc_u)
            add_step(0, 0, None)
            add_step(0, 1, None)
        else:
            add_step(k - 1, 0, 0)
            add_step(k - 1, 1, 0)
            start_down([o for o in range(half, -1, -1) if o % (half - 2) == k % (half - 2)])
    move(0, 0, half)
    move(0, 1, half)
    rest = spare[half - 1:] + [(1, half), (0, half + 1)]
    move(1, *rest.pop(0))
    add_step(half - 1, 0, 0)
    move(1, *rest.pop(0))
    add_step(half - 1, 1, 0)
    done = 0
    move(0, 0, half + 1)
    add_step(half, 0, 0)
    if half > 3:
        add_step(1, 0, 1)
        done = 1
    move(1, *rest.pop(0))
    add_step(half, 1, 0)
    activate(0)
    for o in (half, half - 1):
        for q in group(o):
            for_sib(q, 0)
    move(1, *rest.pop(0))
    for_own(half, 0)
    pass_sum(0, 0, half)
    for q in group(half - 1):
        for_own(q, 0)
    pass_sum(0, 1, half - 1)
    if done:
        add_step(1, 1, 1)
    k = 1 + done
    while rest:
        part, hops = rest.pop(0)
        last = hops - 2 if part == 1 else k
        while k <= last and part == 1:
            add_step(k, 0, 1)
            add_step(k, 1, 1)
            k += 1
        if not rest:
            project(half - 2, 0)
            while k < half:
                add_step(k, 0, 1)
                add_step(k, 1, 1)
                k += 1
        move(1, part, hops)
    add_step(half, 0, 1)
    pass_sum(0, 0, half - 1)
    add_step(half, 1, 1)
    activate(1)
    pass_sum(0, 1, half - 2)
    project(half, 1)
    pass_sum(1, 0, half)
    project(half - 1, 1)
    pass_sum(1, 1, half - 1)
    for o in range(half - 2, 0, -1):
        project(o - 1, 0)
        pass_sum(0, 0, o)
        if o > 1:
            pass_sum(0, 1, o - 1)
        project(o, 1)
        pass_sum(1, 0, o + 1)
        pass_sum(1, 1, o)
    finish(0)
    project(0, 1)
    pass_sum(1, 0, 1)
    finish(1)
    for copy in sends:
        copy.wait_send()


def on_device(n, width, tokens, gate_weight, up_weight, down_weight):
    token_rows, block = tokens.shape
    hidden = gate_weight.shape[1]
    half = n // 2
    slots = 2 * n
    prow = token_rows // 4
    bf16, f32 = jnp.bfloat16, jnp.float32
    dma = pltpu.SemaphoreType.DMA
    ring = (2, half + 1, 4)
    return pl.pallas_call(
        functools.partial(kernel, n, width),
        out_shape=jax.ShapeDtypeStruct((token_rows, block), bf16),
        in_specs=[pl.BlockSpec(memory_space=pl.ANY)] * 4,
        out_specs=pl.BlockSpec(memory_space=pltpu.VMEM),
        scratch_shapes=[
            pltpu.VMEM((slots, token_rows, block), bf16),
            pltpu.VMEM((slots, block, hidden), bf16),
            pltpu.VMEM((slots, block, hidden), bf16),
            pltpu.VMEM((slots, hidden, block), bf16),
            pltpu.VMEM((token_rows, hidden), f32),
            pltpu.VMEM((token_rows, hidden), f32),
            pltpu.VMEM((token_rows, hidden), bf16),
            pltpu.VMEM((n, token_rows, block), f32),
            pltpu.VMEM((n, token_rows, block), bf16),
            pltpu.VMEM((n, token_rows, block), bf16),
            pltpu.VMEM((2, half, 4, prow, block), bf16),
            pltpu.VMEM((2, half, 4, prow, block), bf16),
            dma(()), dma((2, slots)), dma((slots,)),
            dma(ring), dma(ring), dma(ring), dma(ring),
            dma((n, 2)), dma((n, 2)), dma((2, half, 4)), dma((2, half, 4)),
        ],
        compiler_params=pltpu.CompilerParams(
            collective_id=0, has_side_effects=True, vmem_limit_bytes=VMEM_LIMIT
        ),
    )(tokens, gate_weight, up_weight, down_weight)


def solution(mesh):
    n = mesh.shape["gx"] // 2
    spots = {tuple(getattr(dev, "coords", (0, 0, 0)))[:2] for dev in mesh.devices[0]}
    width = len(spots) if len(spots) in (1, 2) else 1
    return jax.shard_map(
        functools.partial(on_device, n, width),
        mesh=mesh,
        in_specs=(P("groups", "gx"), P(None, "gx"), P(None, "gx"), P("gx", None)),
        out_specs=P("groups", "gx"),
        check_vma=False,
    )
```
